32 devices in a mesh: nodes: 32 (over z, y, x, core).
Axes of the slice: x: 2, y: 2, z: 4, core: 2. Of those that a mesh axis runs over, the one named last changes fastest.
Arguments:
- features: bfloat16 [524288, 128], P('nodes'), may hold values from -6 to 6
- nbr_owner: int32 [1024, 32], P('nodes'), may hold values from 0 to 31, all different within a row; in each aligned block of 32 rows (0 to 31, 32 to 63, ...) at most 32 rows name the same one
- nbr_local: int32 [1024, 32], P('nodes'), may hold values from 0 to 16383
- ppr_weight: float32 [1024, 32], P('nodes'), may hold values from 0.01 to 0.1
- labels: int32 [1024], P('nodes'), may hold values from 0 to 171
- w_first: bfloat16 [128, 512], replicated, may hold values from -0.5 to 0.5
- w_second: bfloat16 [512, 512], replicated, may hold values from -0.25 to 0.25
- w_third: bfloat16 [512, 172], replicated, may hold values from -0.25 to 0.25
Outputs:
- loss: float32 [], replicated
- seed_logits: float32 [1024, 172], P('nodes')
- grad_first: float32 [128, 512], replicated
- grad_second: float32 [512, 512], replicated
- grad_third: float32 [512, 172], replicated
The draws below stay inside these ranges and needn't reach their ends.
Inputs may be any that keep to these rules, and one draw needn't show every extreme that they name: `nbr_owner`: each row names 32 different devices; among the rows of one device no device is named by more than 32 rows.
All inputs are finite; a program needn't handle non-finite values.
Results may differ from the reference program's by a relative error of at most 0.01.
The reference program's roundings to bfloat16 on the way count: a program that leaves them out, or rounds other values in their place, can miss the bound.
Values may be sent and summed in bfloat16 or wider, within the bound.
A program may use at most 64 MiB of HBM per device.

```python
import math
import jax
import jax.numpy as jnp
import numpy as np

F = 128
H = 512
C = 172
K = 32
SEED_DEV = 32
NODE_DEV = 16384
CAP = 32
SEEDS = 1024
NODES = 524288
N_NODES = 32


def plant(values, key, least, high):
    longest = values.shape.index(max(values.shape))
    spots = []
    for shift in (0, 1):
        where = [jax.random.randint(jax.random.fold_in(key, axis), (), 0, length) for axis, length in enumerate(values.shape)]
        where[longest] = (where[longest] + shift) % values.shape[longest]
        spots.append(tuple(where))
    return values.at[spots[0]].set(least).at[spots[1]].set(high)


def block_levels(key, shape, split, least, high):
    factor_of, own = 1.0, jax.random.fold_in(key, 6)
    for axis_at, parts in split:
        steps = jnp.exp(jax.random.uniform(jax.random.fold_in(own, axis_at), (parts,), jnp.float32, least / len(split), high / len(split)))
        factor_of = factor_of * jnp.repeat(steps, shape[axis_at] // parts).reshape([-1 if axis == axis_at else 1 for axis in range(len(shape))])
    return factor_of


def assign_block(stream_key, own, number, rows, number_of, top, most, slope):
    order = jax.random.permutation(stream_key, number_of)
    heavy_load, common = shares(number_of, rows * top, most, slope, True), shares(number_of, rows * top, most, slope, False)
    places = jnp.arange(number_of)

    def named(tallies, offset_by):
        used = int((tallies > 0).sum())
        fixed = max(1, used // 4)
        shifted = fixed + (places - fixed + offset_by * (used - fixed)) % max(1, number_of - fixed)
        return jnp.zeros((number_of,), jnp.int32).at[order[jnp.where(places < fixed, places, shifted)]].set(jnp.asarray(tallies, jnp.int32))

    tallies = jnp.where(number % 4 == 0, named(heavy_load, number // 4), named(common, number - number // 4 - 1))
    mixed = jax.random.permutation(jax.random.fold_in(own, 3), number_of)
    giver, receiver = mixed[0:number_of // 2 * 2:2], mixed[1:number_of // 2 * 2:2]
    room = jnp.minimum(tallies[giver] - 1, most - tallies[receiver]) // 2
    room = jnp.where((giver == order[0]) | (receiver == order[0]) | (tallies[receiver] == 0), 0, jnp.maximum(room, 0))
    shifted = jax.random.randint(jax.random.fold_in(own, 4), (number_of // 2,), 0, 1 << 20) % (room + 1)
    tallies = tallies.at[giver].add(-shifted).at[receiver].add(shifted)
    members = jnp.searchsorted(jnp.cumsum(tallies), jnp.arange(rows * top), side="right").astype(jnp.int32)
    grid = members.reshape(top, rows).T
    grid = grid[jax.random.permutation(jax.random.fold_in(own, 1), rows)]
    offset_by = jax.random.randint(jax.random.fold_in(own, 2), (rows, 1), 0, top)
    return jnp.take_along_axis(grid, (jnp.arange(top)[None, :] + offset_by) % top, axis=1)


def shares(number_of, total, most, slope, full):
    loads = [(1 << 20) // math.isqrt(rank ** slope) + 1 for rank in range(1, number_of + 1)]
    largest = most if full else min(most, max(-(-total // number_of), total * loads[0] // sum(loads)))
    least = 1 if total - largest >= number_of - 1 else 0
    given, surplus = [largest] + [least] * (number_of - 1), total - largest - least * (number_of - 1)
    while surplus > 0:
        movable = [i for i in range(1, number_of) if given[i] < largest] or [i for i in range(1, number_of) if given[i] < most]
        whole, budget = sum([loads[i] for i in movable]), surplus
        for i in movable:
            addition = min(most - given[i], max(1, budget * loads[i] // whole), surplus)
            given[i] = given[i] + addition
            surplus = surplus - addition
    return np.array(given)


def noise(rng, shape, spread, limit, split=(), kind=jnp.bfloat16):
    level = block_levels(rng, shape, split, -0.22, 0.18) if split else 1.0
    values = jax.random.normal(rng, shape, jnp.float32) * spread * level
    return jnp.minimum(jnp.maximum(values, -limit), limit).astype(kind)


def setup_inputs(seed: int = 0) -> dict:
    seeds = jax.random.split(jax.random.key(seed), 9)
    features = noise(seeds[0], (NODES, F), 1.0, 6.0, ((0, 32),))
    nbr_owner_keys = jax.random.split(jax.random.fold_in(seeds[1], 1), SEEDS // SEED_DEV)
    nbr_owner_turns = jax.random.permutation(jax.random.fold_in(seeds[1], 3), SEEDS // SEED_DEV)
    nbr_owner = jax.vmap(lambda own, number: assign_block(jax.random.fold_in(seeds[1], 2), own, number, SEED_DEV, N_NODES, K, CAP, 2))(nbr_owner_keys, nbr_owner_turns).reshape((SEEDS, K))
    nbr_local = plant(jax.random.randint(seeds[2], (SEEDS, K), 0, NODE_DEV), jax.random.fold_in(seeds[2], 1), 0, NODE_DEV - 1).astype(jnp.int32)
    ppr_weight = jnp.clip(jnp.exp(math.log(0.1) - 2.3025851 * jax.random.uniform(seeds[3], (SEEDS, K), jnp.float32) ** block_levels(seeds[3], (SEEDS, K), ((0, 32),), -0.2, 0.2)), 0.01, 0.1)
    labels = plant(jax.random.randint(seeds[4], (SEEDS,), 0, C), jax.random.fold_in(seeds[4], 1), 0, C - 1).astype(jnp.int32)
    w_first = noise(seeds[5], (F, H), F ** -0.5, 0.5)
    w_second = noise(seeds[6], (H, H), H ** -0.5, 0.25)
    w_third = noise(seeds[7], (H, C), H ** -0.5, 0.25)
    return {"features": features, "nbr_owner": nbr_owner, "nbr_local": nbr_local, "ppr_weight": ppr_weight, "labels": labels, "w_first": w_first, "w_second": w_second, "w_third": w_third}


def reference(features, nbr_owner, nbr_local, ppr_weight, labels, w_first, w_second, w_third):
    node_index = (nbr_owner * NODE_DEV + nbr_local).reshape(-1).astype(jnp.int32)
    row_block = jnp.take(features, node_index, axis=0)
    first_pre = jnp.dot(row_block, w_first, preferred_element_type=jnp.float32)
    first_act = jnp.maximum(first_pre, 0.0).astype(jnp.bfloat16)
    second_pre = jnp.dot(first_act, w_second, preferred_element_type=jnp.float32)
    second_act = jnp.maximum(second_pre, 0.0).astype(jnp.bfloat16)
    row_logits = jnp.dot(second_act, w_third, preferred_element_type=jnp.float32)
    seed_logits = jnp.sum(ppr_weight[:, :, None] * row_logits.reshape(SEEDS, K, C), axis=1)
    highest = jnp.max(seed_logits, axis=1, keepdims=True)
    log_total = jnp.log(jnp.sum(jnp.exp(seed_logits - highest), axis=1, keepdims=True)) + highest
    onehot = (labels[:, None] == jnp.arange(C, dtype=jnp.int32)[None, :]).astype(jnp.float32)
    loss = jnp.sum(log_total[:, 0] - jnp.sum(onehot * seed_logits, axis=1)) / SEEDS
    logit_grad = (jnp.exp(seed_logits - log_total) - onehot) / SEEDS
    weighted = (ppr_weight[:, :, None] * logit_grad[:, None, :]).astype(jnp.bfloat16).reshape(SEEDS * K, C)
    grad_third = jnp.dot(second_act.T, weighted, preferred_element_type=jnp.float32)
    second_grad = jnp.where(second_pre > 0, jnp.dot(weighted, w_third.T, preferred_element_type=jnp.float32), 0.0).astype(jnp.bfloat16)
    grad_second = jnp.dot(first_act.T, second_grad, preferred_element_type=jnp.float32)
    first_grad = jnp.where(first_pre > 0, jnp.dot(second_grad, w_second.T, preferred_element_type=jnp.float32), 0.0).astype(jnp.bfloat16)
    grad_first = jnp.dot(row_block.T, first_grad, preferred_element_type=jnp.float32)
    return loss, seed_logits, grad_first, grad_second, grad_third
```

```python
import functools

import jax
import jax.numpy as jnp
from jax import lax
from jax.experimental import pallas as pl
from jax.experimental.pallas import tpu as pltpu
from jax.sharding import PartitionSpec as P

MESH = pl.DeviceIdType.MESH
F32 = jnp.float32
BF16 = jnp.bfloat16
LANES = 128


def tdot(a, b):
    return lax.dot_general(a, b, (((0,), (0,)), ((), ())), preferred_element_type=F32)


def dott(a, b):
    return lax.dot_general(a, b, (((1,), (1,)), ((), ())), preferred_element_type=F32)


def kernel(
    dims,
    idx_out, owner, ppr, labels, feats, w1, w2, w3,
    loss_ref, logits_ref, g1_ref, g2_ref, g3_ref,
    feat16, feat32, idx_in, idx_smem, stage, row_send, rows, wbuf, w3p, h1b, h2b,
    zacc, gbuf, loss_in, acc, pair_send, pair_recv, part_send, part_recv, full,
    feat_sem, smem_sem, idx_ss, idx_rs, row_ss, row_rs, loss_ss, loss_rs,
    pair_ss, pair_rs, part_ss, part_rs, full_ss, full_rs, relay_ss, relay_rs,
):
    groups, seeds, classes, per, pieces = dims
    chips = groups // 2
    me = lax.axis_index("nodes")
    chip = me // 2
    core = me % 2
    partner = chip * 2 + (1 - core)
    nodes, feat_dim = feats.shape
    hidden = w1.shape[1]
    padded = w3p.shape[1]
    piece = nodes // pieces

    def remote(src, dst, ss, rs, dev):
        return pltpu.make_async_remote_copy(
            src_ref=src, dst_ref=dst, send_sem=ss, recv_sem=rs, device_id=(dev,), device_id_type=MESH
        )

    def feat_copy(i):
        at = pl.ds(i * piece, piece)
        return pltpu.make_async_copy(feats.at[at], feat16.at[at], feat_sem.at[i])

    for i in range(pieces):
        feat_copy(i).start()

    def others(body, size=groups, mine=me):
        def step(d, carry):
            body(lax.rem(mine + d, size))
            return carry
        lax.fori_loop(1, size, step, 0)

    barrier = pltpu.get_barrier_semaphore()
    others(lambda p: pl.semaphore_signal(barrier, inc=1, device_id=(p,), device_id_type=MESH))
    pl.semaphore_wait(barrier, groups - 1)

    def idx_copy(p, slot):
        return remote(idx_out.at[p], idx_in.at[slot], idx_ss.at[p], idx_rs.at[slot], p)

    others(lambda p: idx_copy(p, me).start())
    idx_in[me] = idx_out[me]

    w3p[...] = jnp.zeros_like(w3p)
    w3p[:, :classes] = w3[...]

    own = owner[...]
    score = ppr[...]

    def weight_step(o, carry):
        w = jnp.sum(jnp.where(own == o, score, 0.0), axis=1, keepdims=True)
        wbuf[pl.ds(pl.multiple_of(o * seeds, 8), seeds), :] = jnp.broadcast_to(w, (seeds, LANES))
        return carry

    lax.fori_loop(0, groups, weight_step, 0)

    block = min(512, piece)
    for i in range(pieces):
        feat_copy(i).wait()

        def widen(j, carry, i=i):
            at = pl.ds(pl.multiple_of(i * piece + j * block, 16), block)
            feat32[at, :] = feat16[at, :].astype(F32)
            return carry

        lax.fori_loop(0, piece // block, widen, 0)

    others(lambda p: idx_copy(p, p).wait_recv())
    to_smem = pltpu.make_async_copy(idx_in, idx_smem, smem_sem)
    to_smem.start()
    to_smem.wait()

    def collect(p):
        for i in range(seeds):
            stage[i : i + 1, :] = feat32[pl.ds(idx_smem[p, 0, i], 1), :]
        return stage[...].astype(BF16)

    def row_copy(p, slot):
        return remote(row_send.at[p], rows.at[slot], row_ss.at[p], row_rs.at[slot], p)

    def send_rows(p):
        row_send[p] = collect(p)
        row_copy(p, me).start()

    others(send_rows)
    rows[me] = collect(me)
    others(lambda p: idx_copy(p, me).wait_send())
    others(lambda p: row_copy(p, p).wait_recv())

    step_owners = min(groups, max(1, 512 // seeds))
    step_rows = step_owners * seeds
    steps = groups // step_owners
    zacc[...] = jnp.zeros_like(zacc)

    def wide(at):
        return jnp.concatenate([wbuf[at, :]] * (padded // LANES), axis=1)

    def forward(t, carry):
        at = pl.ds(pl.multiple_of(t * step_rows, step_rows), step_rows)
        x = rows[pl.ds(t * step_owners, step_owners)].reshape(step_rows, feat_dim)
        h1 = jnp.maximum(jnp.dot(x, w1[...], preferred_element_type=F32), 0.0).astype(BF16)
        h1b[at, :] = h1
        h2 = jnp.maximum(jnp.dot(h1, w2[...], preferred_element_type=F32), 0.0).astype(BF16)
        h2b[at, :] = h2
        z = jnp.dot(h2, w3p[...], preferred_element_type=F32) * wide(at)
        zacc[...] += jnp.sum(z.reshape(step_owners, seeds, padded), axis=0)
        return carry

    lax.fori_loop(0, steps, forward, 0)

    logits = zacc[...]
    logits_ref[...] = logits[:, :classes]
    col = lax.broadcasted_iota(jnp.int32, (seeds, padded), 1)
    valid = col < classes
    highest = jnp.max(jnp.where(valid, logits, -3.0e38), axis=1, keepdims=True)
    expd = jnp.where(valid, jnp.exp(jnp.minimum(logits - highest, 0.0)), 0.0)
    lse = jnp.log(jnp.sum(expd, axis=1, keepdims=True)) + highest
    onehot = jnp.where(col == labels[...], 1.0, 0.0)
    terms = lse - jnp.sum(onehot * logits, axis=1, keepdims=True)
    total = jnp.sum(terms, axis=0, keepdims=True)
    loss_in[me] = jnp.broadcast_to(total, (1, LANES))
    count = float(seeds * groups)
    gbuf[...] = (jnp.where(valid, jnp.exp(jnp.minimum(logits - lse, 0.0)), 0.0) - onehot) / count

    def loss_copy(p, slot):
        return remote(loss_in.at[slot], loss_in.at[slot], loss_ss.at[p], loss_rs.at[slot], p)

    acc[...] = jnp.zeros_like(acc)
    others(lambda p: loss_copy(p, me).start())

    def add_blocks(base, value):
        height = value.shape[0]
        for j in range(value.shape[1] // LANES):
            acc[base + j * height : base + (j + 1) * height, :] += value[:, j * LANES : (j + 1) * LANES]

    base2 = feat_dim * (hidden // LANES)
    base3 = base2 + hidden * (hidden // LANES)

    def backward(t, carry):
        at = pl.ds(pl.multiple_of(t * step_rows, step_rows), step_rows)
        x = rows[pl.ds(t * step_owners, step_owners)].reshape(step_rows, feat_dim)
        h1 = h1b[at, :]
        h2 = h2b[at, :]
        gz = (
            (wide(at).reshape(step_owners, seeds, padded) * gbuf[...][None])
            .reshape(step_rows, padded)
            .astype(BF16)
        )
        add_blocks(base3, tdot(h2, gz))
        d2 = jnp.where(h2 > 0, dott(gz, w3p[...]), 0.0).astype(BF16)
        add_blocks(base2, tdot(h1, d2))
        d1 = jnp.where(h1 > 0, dott(d2, w2[...]), 0.0).astype(BF16)
        add_blocks(0, tdot(x, d1))
        return carry

    lax.fori_loop(0, steps, backward, 0)

    half = chips * per

    def mine(c):
        return pl.ds(pl.multiple_of(core * half + c * per, 16), per)

    def theirs(c):
        return pl.ds(pl.multiple_of((1 - core) * half + c * per, 16), per)

    def chip_order(body):
        others(body, chips, chip)

    def pair_copy(c):
        return remote(pair_send.at[c], pair_recv.at[c], pair_ss.at[c], pair_rs.at[c], partner)

    def send_pair(c):
        pair_send[c] = acc[theirs(c), :].astype(BF16)
        pair_copy(c).start()

    chip_order(send_pair)
    send_pair(chip)

    def part_copy(c, slot):
        return remote(part_send.at[c], part_recv.at[slot], part_ss.at[c], part_rs.at[slot], c * 2 + core)

    def send_part(c):
        pair_copy(c).wait_recv()
        part_send[c] = (acc[mine(c), :] + pair_recv[c].astype(F32)).astype(BF16)
        part_copy(c, chip).start()

    chip_order(send_part)
    pair_copy(chip).wait_recv()
    stage_sum = acc[mine(chip), :] + pair_recv[chip].astype(F32)
    acc[mine(chip), :] = stage_sum

    def add_part(c):
        part_copy(c, c).wait_recv()
        acc[mine(chip), :] += part_recv[c].astype(F32)

    chip_order(add_part)
    full[core, chip] = acc[mine(chip), :].astype(BF16)

    def full_copy(c, slot):
        return remote(full.at[core, slot], full.at[core, slot], full_ss.at[c], full_rs.at[slot], c * 2 + core)

    def relay_copy(c, side):
        return remote(full.at[side, c], full.at[side, c], relay_ss.at[c], relay_rs.at[c], partner)

    chip_order(lambda c: full_copy(c, chip).start())
    relay_copy(chip, core).start()

    others(lambda p: loss_copy(p, p).wait_recv())
    loss_ref[...] = jnp.sum(loss_in[...], axis=0) / count

    def relay(c):
        full_copy(c, c).wait_recv()
        relay_copy(c, core).start()

    chip_order(relay)

    others(lambda p: row_copy(p, me).wait_send())
    others(lambda p: loss_copy(p, me).wait_send())

    def drain(c, carry):
        relay_copy(c, 1 - core).wait_recv()
        relay_copy(c, core).wait_send()
        pair_copy(c).wait_send()
        return carry

    lax.fori_loop(0, chips, drain, 0)
    chip_order(lambda c: part_copy(c, chip).wait_send())
    chip_order(lambda c: full_copy(c, chip).wait_send())

    flat = full[...].reshape(2 * half, LANES)

    def put(out, base, height, width):
        for j in range(-(-width // LANES)):
            cols = min(LANES, width - j * LANES)
            out[:, j * LANES : j * LANES + cols] = flat[base + j * height : base + (j + 1) * height, :cols]

    put(g1_ref, 0, feat_dim, hidden)
    put(g2_ref, base2, hidden, hidden)
    put(g3_ref, base3, hidden, classes)


def on_device(features, nbr_owner, nbr_local, ppr_weight, labels, w_first, w_second, w_third):
    groups = lax.axis_size("nodes")
    seeds, neighbours = nbr_owner.shape
    nodes, feat_dim = features.shape
    hidden, classes = w_third.shape
    padded = -(-classes // LANES) * LANES
    chips = groups // 2
    total = (feat_dim * hidden + hidden * hidden + hidden * padded) // LANES
    per = -(-total // (2 * chips * 16)) * 16
    pieces = 8
    table = jnp.arange(groups, dtype=jnp.int32)
    outgoing = jnp.sum(
        jnp.where(nbr_owner[None] == table[:, None, None], nbr_local[None], 0), axis=2
    )
    outgoing = jnp.pad(outgoing, ((0, 0), (0, LANES - seeds)))[:, None, :]
    dims = (groups, seeds, classes, per, pieces)
    vmem = pl.BlockSpec(memory_space=pltpu.VMEM)
    dma = pltpu.SemaphoreType.DMA
    loss, logits, g1, g2, g3 = pl.pallas_call(
        functools.partial(kernel, dims),
        out_shape=(
            jax.ShapeDtypeStruct((1, LANES), F32),
            jax.ShapeDtypeStruct((seeds, classes), F32),
            jax.ShapeDtypeStruct((feat_dim, hidden), BF16),
            jax.ShapeDtypeStruct((hidden, hidden), BF16),
            jax.ShapeDtypeStruct((hidden, classes), BF16),
        ),
        in_specs=[vmem] * 4 + [pl.BlockSpec(memory_space=pl.ANY)] + [vmem] * 3,
        out_specs=(vmem,) * 5,
        scratch_shapes=[
            pltpu.VMEM((nodes, feat_dim), BF16),
            pltpu.VMEM((nodes, feat_dim), F32),
            pltpu.VMEM((groups, 1, LANES), jnp.int32),
            pltpu.SMEM((groups, 1, LANES), jnp.int32),
            pltpu.VMEM((seeds, feat_dim), F32),
            pltpu.VMEM((groups, seeds, feat_dim), BF16),
            pltpu.VMEM((groups, seeds, feat_dim), BF16),
            pltpu.VMEM((groups * seeds, LANES), F32),
            pltpu.VMEM((hidden, padded), BF16),
            pltpu.VMEM((groups * seeds, hidden), BF16),
            pltpu.VMEM((groups * seeds, hidden), BF16),
            pltpu.VMEM((seeds, padded), F32),
            pltpu.VMEM((seeds, padded), F32),
            pltpu.VMEM((groups, 1, LANES), F32),
            pltpu.VMEM((2 * chips * per, LANES), F32),
            pltpu.VMEM((chips, per, LANES), BF16),
            pltpu.VMEM((chips, per, LANES), BF16),
            pltpu.VMEM((chips, per, LANES), BF16),
            pltpu.VMEM((chips, per, LANES), BF16),
            pltpu.VMEM((2, chips, per, LANES), BF16),
            dma((pieces,)),
            dma(()),
        ]
        + [dma((groups,))] * 6
        + [dma((chips,))] * 8,
        compiler_params=pltpu.CompilerParams(
            collective_id=0, has_side_effects=True, vmem_limit_bytes=60 * 1024 * 1024
        ),
        name="pprgo_step",
    )(outgoing, nbr_owner, ppr_weight, labels[:, None], features, w_first, w_second, w_third)
    return (loss[0, 0], logits, g1.astype(F32), g2.astype(F32), g3.astype(F32))


def solution(mesh):
    return jax.shard_map(
        on_device,
        mesh=mesh,
        in_specs=(
            P("nodes", None),
            P("nodes", None),
            P("nodes", None),
            P("nodes", None),
            P("nodes"),
            P(),
            P(),
            P(),
        ),
        out_specs=(P(), P("nodes", None), P(), P(), P()),
        check_vma=False,
    )
```

```python
import functools

import jax
import jax.numpy as jnp
from jax import lax
from jax.experimental import pallas as pl
from jax.experimental.pallas import tpu as pltpu
from jax.sharding import PartitionSpec as P

MESH = pl.DeviceIdType.MESH
F32 = jnp.float32
BF16 = jnp.bfloat16
LANES = 128


def tdot(a, b):
    return lax.dot_general(a, b, (((0,), (0,)), ((), ())), preferred_element_type=F32)


def dott(a, b):
    return lax.dot_general(a, b, (((1,), (1,)), ((), ())), preferred_element_type=F32)


def kernel(
    dims,
    owner, local, ppr, labels, feats, w1, w2, w3t,
    loss_ref, logits_ref, flat_ref,
    square, idx_out, feat16, feat32, idx_in, idx_smem, stage, row_send, rows, wbuf, w3p, h1b, h2b,
    zacc, gbuf, loss_in, acc, pair_send, pair_recv, part_send, part_recv, full,
    feat_sem, smem_sem, idx_ss, idx_rs, row_ss, row_rs, loss_ss, loss_rs,
    pair_ss, pair_rs, part_ss, part_rs, full_ss, full_rs, relay_ss, relay_rs,
):
    groups, seeds, classes, per, pieces = dims
    chips = groups // 2
    me = lax.axis_index("nodes")
    chip = me // 2
    core = me % 2
    partner = chip * 2 + (1 - core)
    nodes, feat_dim = feats.shape
    hidden = w1.shape[1]
    padded = w3p.shape[0]
    class_rows = -(-classes // 16) * 16
    piece = nodes // pieces

    def remote(src, dst, ss, rs, dev):
        return pltpu.make_async_remote_copy(
            src_ref=src, dst_ref=dst, send_sem=ss, recv_sem=rs, device_id=(dev,), device_id_type=MESH
        )

    def feat_copy(i):
        at = pl.ds(i * piece, piece)
        return pltpu.make_async_copy(feats.at[at], feat16.at[at], feat_sem.at[i])

    for i in range(pieces):
        feat_copy(i).start()

    def others(body, size=groups, mine=me):
        def step(d, carry):
            body(lax.rem(mine + d, size))
            return carry
        lax.fori_loop(1, size, step, 0)

    barrier = pltpu.get_barrier_semaphore()
    others(lambda p: pl.semaphore_signal(barrier, inc=1, device_id=(p,), device_id_type=MESH))

    own = owner[...]
    neighbours = own.shape[1]

    def turned(value, fill):
        square[...] = jnp.full_like(square, fill)
        square[:seeds, :neighbours] = value
        return jnp.transpose(square[...])[:neighbours, :]

    own_t = turned(own, -1)
    local_t = turned(local[...], 0)

    def index_step(o, carry):
        hit = jnp.where(own_t == o, local_t, 0)
        idx_out[o] = jnp.sum(hit, axis=0, keepdims=True)
        return carry

    lax.fori_loop(0, groups, index_step, 0)
    pl.semaphore_wait(barrier, groups - 1)

    def idx_copy(p, slot):
        return remote(idx_out.at[p], idx_in.at[slot], idx_ss.at[p], idx_rs.at[slot], p)

    others(lambda p: idx_copy(p, me).start())
    idx_in[me] = idx_out[me]

    w3p[...] = jnp.zeros_like(w3p)
    w3p[:classes, :] = w3t[...]

    score = ppr[...]

    def weight_step(o, carry):
        w = jnp.sum(jnp.where(own == o, score, 0.0), axis=1, keepdims=True)
        wbuf[pl.ds(pl.multiple_of(o * seeds, 8), seeds), :] = jnp.broadcast_to(w, (seeds, LANES))
        return carry

    lax.fori_loop(0, groups, weight_step, 0)

    block = min(512, piece)
    for i in range(pieces):
        feat_copy(i).wait()

        def widen(j, carry, i=i):
            at = pl.ds(pl.multiple_of(i * piece + j * block, 16), block)
            feat32[at, :] = feat16[at, :].astype(F32)
            return carry

        lax.fori_loop(0, piece // block, widen, 0)

    others(lambda p: idx_copy(p, p).wait_recv())
    to_smem = pltpu.make_async_copy(idx_in, idx_smem, smem_sem)
    to_smem.start()
    to_smem.wait()

    def collect(p):
        for i in range(seeds):
            stage[i : i + 1, :] = feat32[pl.ds(idx_smem[p, 0, i], 1), :]
        return stage[...].astype(BF16)

    def row_copy(p, slot):
        return remote(row_send.at[p], rows.at[slot], row_ss.at[p], row_rs.at[slot], p)

    def send_rows(p):
        row_send[p] = collect(p)
        row_copy(p, me).start()

    others(send_rows)
    rows[me] = collect(me)
    others(lambda p: idx_copy(p, me).wait_send())
    others(lambda p: row_copy(p, p).wait_recv())

    step_owners = min(groups, max(1, 512 // seeds))
    step_rows = step_owners * seeds
    steps = groups // step_owners
    zacc[...] = jnp.zeros_like(zacc)

    def wide(at):
        return jnp.concatenate([wbuf[at, :]] * (padded // LANES), axis=1)

    def forward(t, carry):
        at = pl.ds(pl.multiple_of(t * step_rows, step_rows), step_rows)
        x = rows[pl.ds(t * step_owners, step_owners)].reshape(step_rows, feat_dim)
        h1 = jnp.maximum(jnp.dot(x, w1[...], preferred_element_type=F32), 0.0).astype(BF16)
        h1b[at, :] = h1
        h2 = jnp.maximum(jnp.dot(h1, w2[...], preferred_element_type=F32), 0.0).astype(BF16)
        h2b[at, :] = h2
        z = dott(h2, w3p[...]) * wide(at)
        zacc[...] += jnp.sum(z.reshape(step_owners, seeds, padded), axis=0)
        return carry

    lax.fori_loop(0, steps, forward, 0)

    logits = zacc[...]
    logits_ref[...] = logits[:, :classes]
    col = lax.broadcasted_iota(jnp.int32, (seeds, padded), 1)
    valid = col < classes
    highest = jnp.max(jnp.where(valid, logits, -3.0e38), axis=1, keepdims=True)
    expd = jnp.where(valid, jnp.exp(jnp.minimum(logits - highest, 0.0)), 0.0)
    lse = jnp.log(jnp.sum(expd, axis=1, keepdims=True)) + highest
    eye = lax.broadcasted_iota(jnp.int32, (seeds, seeds), 0) == lax.broadcasted_iota(
        jnp.int32, (seeds, seeds), 1
    )
    label = jnp.sum(jnp.where(eye, labels[...].astype(F32), 0.0), axis=1, keepdims=True)
    onehot = jnp.where(col.astype(F32) == label, 1.0, 0.0)
    terms = lse - jnp.sum(onehot * logits, axis=1, keepdims=True)
    total = jnp.sum(terms, axis=0, keepdims=True)
    loss_in[me] = jnp.broadcast_to(total, (1, LANES))
    count = float(seeds * groups)
    gbuf[...] = (jnp.where(valid, jnp.exp(jnp.minimum(logits - lse, 0.0)), 0.0) - onehot) / count

    def loss_copy(p, slot):
        return remote(loss_in.at[slot], loss_in.at[slot], loss_ss.at[p], loss_rs.at[slot], p)

    acc[...] = jnp.zeros_like(acc)
    others(lambda p: loss_copy(p, me).start())

    def add_blocks(base, value):
        height = value.shape[0]
        for j in range(value.shape[1] // LANES):
            acc[base + j * height : base + (j + 1) * height, :] += value[:, j * LANES : (j + 1) * LANES]

    base2 = feat_dim * (hidden // LANES)
    base3 = base2 + hidden * (hidden // LANES)

    def backward(t, carry):
        at = pl.ds(pl.multiple_of(t * step_rows, step_rows), step_rows)
        x = rows[pl.ds(t * step_owners, step_owners)].reshape(step_rows, feat_dim)
        h1 = h1b[at, :]
        h2 = h2b[at, :]
        gz = (
            (wide(at).reshape(step_owners, seeds, padded) * gbuf[...][None])
            .reshape(step_rows, padded)
            .astype(BF16)
        )
        add_blocks(base3, tdot(gz, h2)[:class_rows])
        d2 = jnp.where(h2 > 0, jnp.dot(gz, w3p[...], preferred_element_type=F32), 0.0).astype(BF16)
        add_blocks(base2, tdot(h1, d2))
        d1 = jnp.where(h1 > 0, dott(d2, w2[...]), 0.0).astype(BF16)
        add_blocks(0, tdot(x, d1))
        return carry

    lax.fori_loop(0, steps, backward, 0)

    half = chips * per

    def mine(c):
        return pl.ds(pl.multiple_of(core * half + c * per, 8), per)

    def theirs(c):
        return pl.ds(pl.multiple_of((1 - core) * half + c * per, 8), per)

    def chip_order(body):
        others(body, chips, chip)

    def pair_copy(c):
        return remote(pair_send.at[c], pair_recv.at[c], pair_ss.at[c], pair_rs.at[c], partner)

    def send_pair(c):
        pair_send[c] = acc[theirs(c), :].astype(BF16)
        pair_copy(c).start()

    chip_order(send_pair)
    send_pair(chip)

    def part_copy(c, slot):
        return remote(part_send.at[c], part_recv.at[slot], part_ss.at[c], part_rs.at[slot], c * 2 + core)

    def send_part(c):
        pair_copy(c).wait_recv()
        part_send[c] = (acc[mine(c), :] + pair_recv[c].astype(F32)).astype(BF16)
        part_copy(c, chip).start()

    chip_order(send_part)
    pair_copy(chip).wait_recv()
    stage_sum = acc[mine(chip), :] + pair_recv[chip].astype(F32)
    acc[mine(chip), :] = stage_sum

    def add_part(c):
        part_copy(c, c).wait_recv()
        acc[mine(chip), :] += part_recv[c].astype(F32)

    chip_order(add_part)
    full[core, chip] = acc[mine(chip), :].astype(BF16)

    def full_copy(c, slot):
        return remote(full.at[core, slot], full.at[core, slot], full_ss.at[c], full_rs.at[slot], c * 2 + core)

    def relay_copy(c, side):
        return remote(full.at[side, c], full.at[side, c], relay_ss.at[c], relay_rs.at[c], partner)

    chip_order(lambda c: full_copy(c, chip).start())
    relay_copy(chip, core).start()

    others(lambda p: loss_copy(p, p).wait_recv())
    loss_ref[...] = jnp.sum(loss_in[...], axis=0) / count

    def relay(c):
        full_copy(c, c).wait_recv()
        relay_copy(c, core).start()

    chip_order(relay)

    others(lambda p: row_copy(p, me).wait_send())
    others(lambda p: loss_copy(p, me).wait_send())

    def drain(c, carry):
        relay_copy(c, 1 - core).wait_recv()
        relay_copy(c, core).wait_send()
        pair_copy(c).wait_send()
        return carry

    lax.fori_loop(0, chips, drain, 0)
    chip_order(lambda c: part_copy(c, chip).wait_send())
    chip_order(lambda c: full_copy(c, chip).wait_send())

    flat_ref[...] = full[...].reshape(2 * half, LANES)


def widen_kernel(loss, logits, flat, loss_ref, logits_ref, g1_ref, g2_ref, g3_ref):
    loss_ref[...] = loss[:, :1]
    logits_ref[...] = logits[...]
    base = 0
    for out in (g1_ref, g2_ref, g3_ref):
        height, width = out.shape
        stride = -(-height // 16) * 16
        for j in range(width // LANES):
            out[:, j * LANES : (j + 1) * LANES] = flat[base : base + height, :].astype(F32)
            base += stride


def on_device(features, nbr_owner, nbr_local, ppr_weight, labels, w_first, w_second, w_third):
    groups = lax.axis_size("nodes")
    seeds, neighbours = nbr_owner.shape
    nodes, feat_dim = features.shape
    hidden, classes = w_third.shape
    padded = -(-classes // LANES) * LANES
    chips = groups // 2
    class_rows = -(-classes // 16) * 16
    total = (feat_dim + hidden + class_rows) * (hidden // LANES)
    per = -(-total // (2 * chips * 8)) * 8
    pieces = 8
    dims = (groups, seeds, classes, per, pieces)
    vmem = pl.BlockSpec(memory_space=pltpu.VMEM)
    dma = pltpu.SemaphoreType.DMA
    loss, logits, flat = pl.pallas_call(
        functools.partial(kernel, dims),
        out_shape=(
            jax.ShapeDtypeStruct((1, LANES), F32),
            jax.ShapeDtypeStruct((seeds, classes), F32),
            jax.ShapeDtypeStruct((2 * chips * per, LANES), BF16),
        ),
        in_specs=[vmem] * 4 + [pl.BlockSpec(memory_space=pl.ANY)] + [vmem] * 3,
        out_specs=(vmem,) * 3,
        scratch_shapes=[
            pltpu.VMEM((LANES, LANES), jnp.int32),
            pltpu.VMEM((groups, 1, LANES), jnp.int32),
            pltpu.VMEM((nodes, feat_dim), BF16),
            pltpu.VMEM((nodes, feat_dim), F32),
            pltpu.VMEM((groups, 1, LANES), jnp.int32),
            pltpu.SMEM((groups, 1, LANES), jnp.int32),
            pltpu.VMEM((seeds, feat_dim), F32),
            pltpu.VMEM((groups, seeds, feat_dim), BF16),
            pltpu.VMEM((groups, seeds, feat_dim), BF16),
            pltpu.VMEM((groups * seeds, LANES), F32),
            pltpu.VMEM((padded, hidden), BF16),
            pltpu.VMEM((groups * seeds, hidden), BF16),
            pltpu.VMEM((groups * seeds, hidden), BF16),
            pltpu.VMEM((seeds, padded), F32),
            pltpu.VMEM((seeds, padded), F32),
            pltpu.VMEM((groups, 1, LANES), F32),
            pltpu.VMEM((2 * chips * per, LANES), F32),
            pltpu.VMEM((chips, per, LANES), BF16),
            pltpu.VMEM((chips, per, LANES), BF16),
            pltpu.VMEM((chips, per, LANES), BF16),
            pltpu.VMEM((chips, per, LANES), BF16),
            pltpu.VMEM((2, chips, per, LANES), BF16),
            dma((pieces,)),
            dma(()),
        ]
        + [dma((groups,))] * 6
        + [dma((chips,))] * 8,
        compiler_params=pltpu.CompilerParams(
            collective_id=0, has_side_effects=True, vmem_limit_bytes=60 * 1024 * 1024
        ),
        name="pprgo_step",
    )(
        nbr_owner, nbr_local, ppr_weight, labels.reshape(1, seeds), features,
        w_first, w_second, w_third.T,
    )
    loss, logits, g1, g2, g3 = pl.pallas_call(
        widen_kernel,
        out_shape=(
            jax.ShapeDtypeStruct((1, 1), F32),
            jax.ShapeDtypeStruct((seeds, classes), F32),
            jax.ShapeDtypeStruct((feat_dim, hidden), F32),
            jax.ShapeDtypeStruct((hidden, hidden), F32),
            jax.ShapeDtypeStruct((classes, hidden), F32),
        ),
        in_specs=[vmem] * 3,
        out_specs=(vmem,) * 5,
        name="widen",
    )(loss, logits, flat)
    return (loss.reshape(()), logits, g1, g2, g3.T)


def solution(mesh):
    return jax.shard_map(
        on_device,
        mesh=mesh,
        in_specs=(
            P("nodes", None),
            P("nodes", None),
            P("nodes", None),
            P("nodes", None),
            P("nodes"),
            P(),
            P(),
            P(),
        ),
        out_specs=(P(), P("nodes", None), P(), P(), P()),
        check_vma=False,
    )
```
